32 devices in a mesh: samp: 16 (over z, y, core), var: 2 (over x).
Axes of the slice: x: 2, y: 2, z: 4, core: 2. Of those that a mesh axis runs over, the one named last changes fastest.
Arguments:
- dosages: bfloat16 [8192, 3584], P('samp', 'var'), may hold values from 0 to 2
- weights: bfloat16 [3584, 512], P('var'), may hold values from -0.09375 to 0.09375
- prior: float32 [8192, 512], P('samp', 'var'), may hold values from -6 to 6
- cohort: int32 [8192, 1], P('samp'), may hold values from 0 to 15
- expression: bfloat16 [8192, 10240], P('samp', 'var'), may hold values from -6 to 6
Outputs:
- correlation: float32 [512, 10240], P('samp', 'var')
The draws below stay inside these ranges and needn't reach their ends.
Inputs may be any that keep to these rules, and one draw needn't show every extreme that they name: Every cohort has at least one sample.
All inputs are finite; a program needn't handle non-finite values.
Results may differ from the reference program's by a relative error of at most 0.0042.
Values may be sent and summed in bfloat16 or wider, within the bound.
No kernel may reach another device: no remote copies, remote signals or barrier semaphores. Data moves between devices by JAX's collectives and lax.ppermute only.
A program may use at most 64 MiB of HBM per device.

```python
import jax
import jax.numpy as jnp
from jax import lax

K = 512
GENES = 10240
COHORTS = 16
SAMPLES = 8192
VARIANTS = 3584


def with_spikes(result, rng, source, target, blocks, factor):
    owner, partner = [(jnp.arange(result.shape[dim]) // (result.shape[dim] // blocks)).reshape([-1 if axis == dim else 1 for axis in range(result.ndim)]) for dim in (source, target)]
    chosen = jax.random.permutation(rng, blocks)[partner]
    strong = (owner == chosen) | (owner == (partner + blocks // 2) % blocks)
    return jnp.where(strong, factor * result, result)


def steps_of(rng, extent, cuts, least, high):
    def one(dim, shards_of):
        steps = jax.random.uniform(jax.random.fold_in(jax.random.fold_in(rng, 6), dim), (shards_of,), jnp.float32, least / len(cuts), high / len(cuts))
        return jnp.repeat(jnp.exp(steps), extent[dim] // shards_of).reshape((-1,) + (1,) * (len(extent) - dim - 1))

    gain = one(*cuts[0])
    for cut in cuts[1:]:
        gain = gain * one(*cut)
    return gain


def different_ones(key, rows, number_of, top, lift):
    order = jax.random.permutation(jax.random.fold_in(key, 1), number_of)
    favour = order
    for power in range(3):
        favour = favour * favour // number_of
    favour = favour * lift // number_of
    chance = jax.random.randint(jax.random.fold_in(key, 2), (rows, number_of), 0, 4096) + favour
    fixed_rows = jax.random.permutation(jax.random.fold_in(key, 3), rows)[jnp.arange(number_of) % rows]
    chance = jnp.where(jnp.arange(rows)[:, None] == fixed_rows[None, :], 1 << 14, chance)
    merit = chance * number_of + jnp.arange(number_of)
    return lax.top_k(merit.astype(jnp.int32), top)[1].astype(jnp.int32)


def scatter_about(key, shape, scale, bound, split=(), kind=jnp.bfloat16):
    gain = steps_of(key, shape, split, -0.22, 0.18) if split else 1.0
    drawn = jax.random.normal(key, shape, jnp.float32) * scale * gain
    return jnp.minimum(jnp.maximum(drawn, -bound), bound).astype(kind)


def noise_with(own_key, dims, scale, bound, cuts, heavy, kind=jnp.bfloat16):
    result = scale * jax.random.normal(own_key, dims, jnp.float32)
    if cuts:
        result = result * steps_of(own_key, dims, cuts, -0.22, 0.18)
    return jnp.clip(with_spikes(result, jax.random.fold_in(own_key, 3), *heavy), -bound, bound).astype(kind)


def setup_inputs(seed: int = 0) -> dict:
    splits = jax.random.split(jax.random.key(seed), 6)
    return {
        "dosages": jnp.clip(2.0 * jax.random.uniform(splits[0], (SAMPLES, VARIANTS), jnp.float32) ** steps_of(splits[0], (SAMPLES, VARIANTS), ((0, 16), (1, 2)), -0.2, 0.2), 0.0, 2.0).astype(jnp.bfloat16),
        "weights": scatter_about(splits[1], (VARIANTS, K), VARIANTS ** -0.5, 0.09375, ((0, 2),)),
        "prior": noise_with(splits[2], (SAMPLES, K), 1.0, 6.0, ((0, 16), (1, 2)), (0, 1, 16, 2.0), jnp.float32),
        "cohort": different_ones(splits[3], SAMPLES, COHORTS, 1, 512),
        "expression": scatter_about(splits[4], (SAMPLES, GENES), 1.0, 6.0, ((0, 16), (1, 2))),
    }


def reference(dosages, weights, prior, cohort, expression):
    scores = prior + jnp.dot(dosages, weights, preferred_element_type=jnp.float32)
    onehot = (cohort == jnp.arange(COHORTS, dtype=jnp.int32)[None, :]).astype(jnp.float32)
    counts = lax.optimization_barrier(jnp.sum(onehot, axis=0))
    sums = jnp.dot(onehot.T, scores, precision=lax.Precision.HIGHEST)
    means = sums / counts[:, None]
    centered = scores - means[cohort[:, 0]]
    spread = lax.rsqrt(lax.optimization_barrier(jnp.sum(centered * centered, axis=0)) / SAMPLES + 1e-06)
    standard = (centered * spread[None, :]).astype(jnp.bfloat16)
    cross = jnp.dot(standard.T, expression, preferred_element_type=jnp.float32)
    return cross / SAMPLES
```

```python
import jax
import jax.numpy as jnp
from jax import lax
from jax.sharding import PartitionSpec as P

COHORTS = 16
GENE_CHUNKS = 2
BF16, F32 = jnp.bfloat16, jnp.float32
EXACT = lax.Precision.HIGHEST


def flip(size, stride):
    return [(i, i ^ stride) for i in range(size)]


def shift(size, step):
    return [(i, (i + step) % size) for i in range(size)]


def strides(size):
    return [1 << bit for bit in range(size.bit_length() - 1)]


def pick(array, index, axis):
    return lax.dynamic_index_in_dim(array, index, axis, keepdims=False)


def all_sum(value, size):
    for stride in strides(size):
        value = value + lax.ppermute(value, "samp", flip(size, stride))
    return value


def scatter_sum(standard, expression, place, size):
    owners, rows, samples = standard.shape

    def product(lhs):
        return lax.dot_general(
            lhs, expression, (((2,), (0,)), ((), ())), preferred_element_type=F32
        )

    halves = standard.reshape(owners // 2, 2, rows, samples)
    bit = place & 1
    sent = product(pick(halves, 1 - bit, 1)).astype(BF16)
    total = product(pick(halves, bit, 1)) + lax.ppermute(sent, "samp", flip(size, 1)).astype(F32)
    for stride in strides(size)[1:]:
        bit = (place // stride) & 1
        halves = total.reshape(total.shape[0] // 2, 2, rows, -1)
        sent = pick(halves, 1 - bit, 1).astype(BF16)
        total = pick(halves, bit, 1) + lax.ppermute(sent, "samp", flip(size, stride)).astype(F32)
    return total[0]


def shards(dosages, weights, prior, cohort, expression, *, size, parts):
    place, part = lax.axis_index("samp"), lax.axis_index("var")
    samples, width = prior.shape
    rows = width // size
    genes = expression.shape[1]

    scores = lax.dot_general(
        weights, dosages, (((0,), (1,)), ((), ())), preferred_element_type=F32
    ).reshape(size, parts, rows, samples)
    at = part * (size // parts)
    own = lax.dynamic_slice_in_dim(scores, at, size // parts, 0)
    own = own + prior.T.reshape(size // parts, parts, rows, samples)
    scores = lax.dynamic_update_slice_in_dim(scores, own, at, 0)

    member = cohort[:, 0][None, :] == jnp.arange(COHORTS, dtype=jnp.int32)[:, None]
    member = member.astype(F32)
    counts = jnp.sum(member, axis=1)

    def cohort_sums(values):
        return lax.dot_general(
            member, values.reshape(size * rows, samples), (((1,), (1,)), ((), ())), precision=EXACT
        )

    scored = pick(scores, part, 1)
    sums = cohort_sums(scored)
    for step in range(1, parts):
        values = pick(scores, (part + step) % parts, 1)
        offset = jnp.mean(values, axis=2, keepdims=True)
        small = jnp.concatenate([cohort_sums(values), offset.reshape(1, -1)], axis=0)
        small = lax.ppermute(small, "var", shift(parts, step))
        sums = sums + small[:COHORTS]
        values = lax.ppermute((values - offset).astype(BF16), "var", shift(parts, step))
        scored = scored + values.astype(F32) + small[COHORTS].reshape(size, rows, 1)
    small = jnp.concatenate(
        [sums, jnp.broadcast_to(counts[:, None], (COHORTS, 128))], axis=1
    )
    small = all_sum(small, size)
    sums, counts = small[:, :-128], small[:, -1]
    means = sums / counts[:, None]
    total = jnp.sum(counts)
    centered = scored - lax.dot_general(
        means, member, (((0,), (0,)), ((), ())), precision=EXACT
    ).reshape(scored.shape)

    standard = [centered.astype(BF16)]
    squares = [jnp.sum(centered * centered, axis=2)]
    for step in range(1, parts):
        standard.append(lax.ppermute(standard[0], "var", shift(parts, step)))
        wide = standard[step].astype(F32)
        squares.append(jnp.sum(wide * wide, axis=2))
    chunk = genes // GENE_CHUNKS
    sums = [
        [
            scatter_sum(values, expression[:, at : at + chunk], place, size)
            for at in range(0, genes, chunk)
        ]
        for values in standard
    ]
    squares = all_sum(jnp.stack(squares), size)
    spread = pick(lax.rsqrt(squares / total + 1e-06) / total, place, 1)
    result = jnp.zeros((parts, rows, genes), F32)
    for step in range(parts):
        values = jnp.concatenate(sums[step], axis=1) * spread[step][:, None]
        result = lax.dynamic_update_slice_in_dim(
            result, values[None], (part - step) % parts, 0
        )
    return result.reshape(parts * rows, genes)


def solution(mesh):
    size, parts = mesh.shape["samp"], mesh.shape["var"]

    def step(*arrays):
        return shards(*arrays, size=size, parts=parts)

    placed = (P("samp", "var"), P("var", None), P("samp", "var"), P("samp", None), P("samp", "var"))
    return jax.shard_map(
        step, mesh=mesh, in_specs=placed, out_specs=P("samp", "var"), check_vma=False
    )
```

```python
import functools

import jax
import jax.numpy as jnp
from jax import lax
from jax.experimental import pallas as pl
from jax.experimental.pallas import tpu as pltpu
from jax.sharding import PartitionSpec as P


COHORTS = 16
LANES = 128
BF16, F32 = jnp.bfloat16, jnp.float32
EXACT = lax.Precision.HIGHEST


def flip(size, stride):
    return [(i, i ^ stride) for i in range(size)]


def shift(size, step):
    return [(i, (i + step) % size) for i in range(size)]


def strides(size):
    return [1 << bit for bit in range(size.bit_length() - 1)]


def pick(array, index, axis):
    return lax.dynamic_index_in_dim(array, index, axis, keepdims=False)


def in_hbm(array):
    return pltpu.with_memory_space_constraint(array, pltpu.HBM)


def all_sum(value, size):
    for stride in strides(size):
        value = value + lax.ppermute(value, "samp", flip(size, stride))
    return value


def member_of(cohort, kind=F32):
    shape = (COHORTS, cohort.shape[-1])
    return (cohort == lax.broadcasted_iota(jnp.int32, shape, 0)).astype(kind)


def cohort_sums(member, values):
    values = values.reshape(-1, values.shape[-1])
    return lax.dot_general(
        member, values, (((1,), (1,)), ((), ())), precision=EXACT, preferred_element_type=F32
    )


def of_members(table, member):
    return lax.dot_general(
        table, member, (((0,), (0,)), ((), ())), precision=EXACT, preferred_element_type=F32
    )


def thirds(values):
    high = values.astype(BF16)
    values = values - high.astype(F32)
    mid = values.astype(BF16)
    return high, mid, (values - mid.astype(F32)).astype(BF16)


def score_kernel(cuts, where_ref, weights_ref, dosages_ref, prior_ref, cohort_ref, *refs):
    *refs, weights, dosages, prior, cohort, acc, sems = refs
    part = where_ref[1]
    size, parts, rows, samples = acc.shape
    share = size // parts
    (own_ref, *sent_refs), sums_refs = refs[:parts], refs[parts:]
    width = size * rows
    copies = []
    for k, (at, count) in enumerate(cuts):
        copies.append(
            (
                pltpu.make_async_copy(
                    weights_ref.at[pl.ds(at, count)], weights.at[pl.ds(at, count)], sems.at[0, k]
                ),
                pltpu.make_async_copy(
                    dosages_ref.at[:, pl.ds(at, count)],
                    dosages.at[:, pl.ds(at, count)],
                    sems.at[1, k],
                ),
            )
        )
        copies[k][0].start()
        copies[k][1].start()
    extra = pltpu.make_async_copy(prior_ref, prior, sems.at[2, 0])
    extra.start()
    known = pltpu.make_async_copy(cohort_ref, cohort, sems.at[2, 1])
    known.start()
    for k, (at, count) in enumerate(cuts):
        copies[k][0].wait()
        copies[k][1].wait()
        product = lax.dot_general(
            weights[pl.ds(at, count)],
            dosages[:, pl.ds(at, count)],
            (((0,), (1,)), ((), ())),
            preferred_element_type=F32,
        ).reshape(acc.shape)
        if k == 0:
            acc[...] = product
        else:
            acc[...] += product
    known.wait()
    member = member_of(cohort[...], BF16)
    extra.wait()
    acc[pl.ds(part * share, share)] += prior[...].T.reshape(share, parts, rows, samples)

    def sums_of(values):
        pieces = thirds(values.reshape(size * rows, samples))
        return sum(
            lax.dot_general(member, x, (((1,), (1,)), ((), ())), preferred_element_type=F32)
            for x in pieces
        )

    values = acc[:, part]
    own_ref[...] = values
    sums_refs[0][:, :width] = sums_of(values)
    counts = jnp.sum(member.astype(F32), axis=1, keepdims=True)
    sums_refs[0][:, width:] = jnp.broadcast_to(counts, (COHORTS, LANES))
    for other in range(1, parts):
        values = acc[:, lax.rem(part + other, parts)]
        sums_refs[other][:, :width] = sums_of(values)
        sums_refs[other][:, width:] = jnp.zeros((COHORTS, LANES), F32)
        mean = jnp.mean(values, axis=2, keepdims=True)
        sent_refs[other - 1][...] = (values - mean).astype(BF16)


def center_kernel(own_ref, total_ref, cohort_ref, *refs):
    *others, out_ref = refs
    size, rows, samples = own_ref.shape
    width = size * rows
    table = -total_ref[:, :width] / total_ref[:, width : width + 1]
    scores = own_ref[...]
    for got_ref, theirs_ref in zip(others[::2], others[1::2]):
        scores += got_ref[...].astype(F32)
        table += jnp.sum(theirs_ref[:, :width], axis=0, keepdims=True) / samples
    member = member_of(cohort_ref[...], BF16)
    scores += lax.dot_general(
        jnp.concatenate(thirds(table), axis=0),
        jnp.concatenate([member] * 3, axis=0),
        (((0,), (0,)), ((), ())),
        preferred_element_type=F32,
    ).reshape(scores.shape)
    out_ref[...] = scores.astype(BF16)


def local_scores(dosages, weights, prior, cohort, where, size, parts):
    samples, variants = dosages.shape
    width = prior.shape[1]
    rows = width // size
    if rows % 16 == 0 and samples % LANES == 0 and variants % 256 == 0:
        step = min(512, variants)
        cuts = [(at, min(step, variants - at)) for at in range(0, variants, step)]
        vmem = pl.BlockSpec(memory_space=pltpu.VMEM)
        hbm = pl.BlockSpec(memory_space=pltpu.HBM)
        part_shape = (size, rows, samples)
        out = pl.pallas_call(
            functools.partial(score_kernel, cuts),
            out_shape=[
                pltpu.VMEM(part_shape, F32),
                *[pltpu.VMEM(part_shape, BF16)] * (parts - 1),
                *[pltpu.VMEM((COHORTS, width + LANES), F32)] * parts,
            ],
            in_specs=[pl.BlockSpec(memory_space=pltpu.SMEM), hbm, hbm, hbm, hbm],
            out_specs=[vmem] * (2 * parts),
            scratch_shapes=[
                pltpu.VMEM((variants, width * parts), BF16),
                pltpu.VMEM((samples, variants), BF16),
                pltpu.VMEM((samples, width), F32),
                pltpu.VMEM((1, samples), jnp.int32),
                pltpu.VMEM((size, parts, rows, samples), F32),
                pltpu.SemaphoreType.DMA((3, len(cuts))),
            ],
            compiler_params=pltpu.CompilerParams(vmem_limit_bytes=16 << 20),
            name="scores",
        )(where, *map(in_hbm, (weights, dosages, prior, cohort)))
        return out[0], out[1:parts], out[parts:]
    part = where[1]
    scores = lax.dot_general(
        weights, dosages, (((0,), (1,)), ((), ())), preferred_element_type=F32
    ).reshape(size, parts, rows, samples)
    at = part * (size // parts)
    own = lax.dynamic_slice_in_dim(scores, at, size // parts, 0)
    own = own + prior.T.reshape(size // parts, parts, rows, samples)
    scores = lax.dynamic_update_slice_in_dim(scores, own, at, 0)
    by_part = [pick(scores, (part + other) % parts, 1) for other in range(parts)]
    member = member_of(cohort)
    counts = jnp.broadcast_to(jnp.sum(member, axis=1, keepdims=True), (COHORTS, LANES))
    sums = [
        jnp.concatenate([cohort_sums(member, x), counts * (k == 0)], axis=1)
        for k, x in enumerate(by_part)
    ]
    sent = [(x - jnp.mean(x, axis=2, keepdims=True)).astype(BF16) for x in by_part[1:]]
    return by_part[0], sent, sums


def center(own, got, theirs, total, cohort):
    size, rows, samples = own.shape
    if rows % 16 == 0 and samples % LANES == 0:
        others = [x for pair in zip(got, theirs) for x in pair]
        return pl.pallas_call(
            center_kernel,
            out_shape=pltpu.VMEM(own.shape, BF16),
            compiler_params=pltpu.CompilerParams(vmem_limit_bytes=8 << 20),
            name="center",
        )(own, total, cohort, *others)
    width = size * rows
    table = -total[:, :width] / total[:, width : width + 1]
    table = table + jnp.sum(sum(theirs)[:, :width], axis=0)[None, :] / samples
    table = of_members(table, member_of(cohort)).reshape(own.shape)
    return (own + sum(x.astype(F32) for x in got) + table).astype(BF16)


def stage_kernel(source_ref, out_ref, sem):
    copy = pltpu.make_async_copy(source_ref, out_ref, sem)
    copy.start()
    copy.wait()


def stage(array):
    if array.size * array.dtype.itemsize > 6 << 20:
        return array
    return pl.pallas_call(
        stage_kernel,
        out_shape=pltpu.VMEM(array.shape, array.dtype),
        in_specs=[pl.BlockSpec(memory_space=pltpu.HBM)],
        out_specs=pl.BlockSpec(memory_space=pltpu.VMEM),
        scratch_shapes=[pltpu.SemaphoreType.DMA],
        compiler_params=pltpu.CompilerParams(vmem_limit_bytes=1 << 20),
        name="stage",
    )(in_hbm(array))


def product_kernel(cuts, squares, where_ref, standard_ref, expression_ref, sent_ref, mine_ref):
    bit = where_ref[0] & 1
    half, _, rows, samples = standard_ref.shape
    sent = standard_ref[:, 1 - bit].reshape(half * rows, samples)
    mine = standard_ref[:, bit].reshape(half * rows, samples)
    if squares:
        end = sum(cuts[-1][::2])
        first = lax.broadcasted_iota(jnp.int32, (half * rows, LANES), 1) < LANES // 2
        total = jnp.sum(sent.astype(F32) ** 2, axis=1, keepdims=True)
        high = total.astype(BF16).astype(F32)
        sent_ref[:, end:] = jnp.where(first, high, total - high).astype(BF16)
        total = jnp.sum(mine.astype(F32) ** 2, axis=1, keepdims=True)
        mine_ref[:, end:] = jnp.where(first, total, 0.0)
    both = jnp.concatenate([sent, mine], axis=0)
    for at, start, count in cuts:
        block = expression_ref[:, start : start + count]
        total = jnp.dot(both, block, preferred_element_type=F32)
        sent_ref[:, at : at + count] = total[: half * rows].astype(BF16)
        mine_ref[:, at : at + count] = total[half * rows :]


def products(standard, expression, where, at, count, squares):
    size, rows, samples = standard.shape
    halves = standard.reshape(size // 2, 2, rows, samples)
    if rows % 16 == 0 and samples % LANES == 0 and count % LANES == 0:
        step = 512
        cuts = [(k, at + k, min(step, count - k)) for k in range(0, count, step)]
        shape = (size // 2 * rows, count + LANES * squares)
        vmem = pl.BlockSpec(memory_space=pltpu.VMEM)
        return pl.pallas_call(
            functools.partial(product_kernel, cuts, squares),
            out_shape=[pltpu.VMEM(shape, BF16), pltpu.VMEM(shape, F32)],
            in_specs=[pl.BlockSpec(memory_space=pltpu.SMEM), vmem, vmem],
            out_specs=[vmem, vmem],
            compiler_params=pltpu.CompilerParams(vmem_limit_bytes=12 << 20),
        )(where, halves, expression)
    expression = expression[:, at : at + count]
    results = []
    place = where[0]
    for k in (1 - place & 1, place & 1):
        lhs = pick(halves, k, 1).reshape(-1, samples)
        result = jnp.dot(lhs, expression, preferred_element_type=F32)
        if squares:
            total = jnp.sum(lhs.astype(F32) ** 2, axis=1, keepdims=True)
            total = jnp.broadcast_to(total, (total.shape[0], LANES))
            first = jnp.arange(LANES) < LANES // 2
            if not results:
                high = lax.reduce_precision(total, 8, 7)
                total = jnp.where(first, high, total - high)
            else:
                total = jnp.where(first, total, 0.0)
            result = jnp.concatenate([result, total], axis=1)
        results.append(result)
    return results[0].astype(BF16), results[1]


def fold_kernel(shift, where_ref, mine_ref, got_ref, sent_ref, kept_ref):
    bit = (where_ref[0] >> shift) & 1
    sent_ref[...] = (mine_ref[:, 1 - bit] + got_ref[:, 1 - bit].astype(F32)).astype(BF16)
    kept_ref[...] = mine_ref[:, bit] + got_ref[:, bit].astype(F32)


def fold(mine, got, where, stride):
    before, _, rows, width = mine.shape
    if rows % 16 == 0 and width % LANES == 0:
        vmem = pl.BlockSpec(memory_space=pltpu.VMEM)
        return pl.pallas_call(
            functools.partial(fold_kernel, stride.bit_length() - 1),
            out_shape=[pltpu.VMEM((before, rows, width), kind) for kind in (BF16, F32)],
            in_specs=[pl.BlockSpec(memory_space=pltpu.SMEM), vmem, vmem],
            out_specs=[vmem, vmem],
            compiler_params=pltpu.CompilerParams(vmem_limit_bytes=4 << 20),
        )(where, mine, got)
    total = mine + got.astype(F32)
    bit = (where[0] // stride) & 1
    return pick(total, 1 - bit, 1).astype(BF16), pick(total, bit, 1)


def scatter_sum(standard, expression, where, size, chunk):
    at, count, order = chunk
    rows = standard.shape[1]
    sent, mine = products(standard, expression, where, at, count, at == 0)
    width = sent.shape[1]
    left = strides(size)[::-1]
    for stride, coming in zip(order, [*order[1:], None]):
        left.remove(stride)
        got = lax.ppermute(sent, "samp", flip(size, stride))
        if coming is None:
            return mine.reshape(rows, width), got.reshape(rows, width)
        axis = left.index(coming)
        shape = (2**axis, 2, 2 ** (len(left) - axis - 1) * rows, width)
        sent, mine = fold(mine.reshape(shape), got.reshape(shape), where, coming)


def finish_kernel(plan, everyone, where_ref, *refs):
    *refs, out_ref = refs
    parts = len(plan)
    terms = iter(zip(refs[::2], refs[1::2]))
    for k, chunks in enumerate(plan):
        part = lax.rem(where_ref[1] + parts - k, parts)
        for at, count, _ in chunks:
            mine, got = next(terms)
            total = mine[...] + got[...].astype(F32)
            if at == 0:
                middle = count + LANES // 2
                squares = total[:, count : count + 1] + total[:, middle : middle + 1]
                spread = lax.rsqrt(squares / everyone + 1e-06) / everyone
            out_ref[part, :, at : at + count] = total[:, :count] * spread


def finish(cross, plan, where, everyone):
    rows = cross[0][0].shape[0]
    genes = sum(chunk[1] for chunk in plan[0])
    parts = len(plan)
    if rows % 16 == 0:
        vmem = pl.BlockSpec(memory_space=pltpu.VMEM)
        return pl.pallas_call(
            functools.partial(finish_kernel, plan, everyone),
            out_shape=jax.ShapeDtypeStruct((parts, rows, genes), F32),
            in_specs=[pl.BlockSpec(memory_space=pltpu.SMEM), *[vmem] * (2 * len(cross))],
            out_specs=vmem,
            compiler_params=pltpu.CompilerParams(vmem_limit_bytes=12 << 20),
            name="finish",
        )(where, *[x for pair in cross for x in pair])
    result = jnp.zeros((parts, rows, genes), F32)
    cross = iter([mine + got.astype(F32) for mine, got in cross])
    for k, chunks in enumerate(plan):
        totals = [next(cross) for _ in chunks]
        count = chunks[0][1]
        squares = totals[0][:, count] + totals[0][:, count + LANES // 2]
        spread = lax.rsqrt(squares / everyone + 1e-06) / everyone
        values = jnp.concatenate([totals[0][:, :count], *totals[1:]], axis=1) * spread[:, None]
        result = lax.dynamic_update_slice_in_dim(result, values[None], (where[1] - k) % parts, 0)
    return result


def chunk_plan(size, parts, genes):
    near = strides(size)
    late = [near[0], near[2], near[1], *near[3:]] if size >= 8 else near
    tiles = genes // LANES
    cut = tiles * 11 // 20 * LANES
    plan = [[(0, cut, near), (cut, genes - cut, near)]]
    for _ in range(1, parts):
        cut = tiles * 2 // 5 * LANES
        plan.append([(0, cut, near), (cut, genes - cut, late)])
    return plan


def shards(dosages, weights, prior, cohort, expression, *, size, parts):
    where = jnp.stack([lax.axis_index("samp"), lax.axis_index("var")]).astype(jnp.int32)
    samples, width = prior.shape
    rows = width // size
    genes = expression.shape[1]
    cohort = cohort.reshape(1, samples)

    own, sent, sums = local_scores(dosages, weights, prior, cohort, where, size, parts)
    theirs = [lax.ppermute(sums[k], "var", shift(parts, k)) for k in range(1, parts)]
    got = [lax.ppermute(sent[k - 1], "var", shift(parts, k)) for k in range(1, parts)]
    total = all_sum(sum(theirs, sums[0]), size)
    if rows % 16 == 0:
        expression = stage(expression)

    standard = [center(own, got, theirs, total, cohort)]
    for k in range(1, parts):
        standard.append(lax.ppermute(standard[0], "var", shift(parts, k)))

    plan = chunk_plan(size, parts, genes)
    cross = [
        scatter_sum(standard[k], expression, where, size, chunk)
        for k, chunks in enumerate(plan)
        for chunk in chunks
    ]
    return finish(cross, plan, where, samples * size).reshape(parts * rows, genes)


def solution(mesh):
    size, parts = mesh.shape["samp"], mesh.shape["var"]
    placed = (P("samp", "var"), P("var", None), P("samp", "var"), P("samp", None), P("samp", "var"))
    return jax.shard_map(
        functools.partial(shards, size=size, parts=parts),
        mesh=mesh,
        in_specs=placed,
        out_specs=P("samp", "var"),
        check_vma=False,
    )
```

```python
import functools

import jax
import jax.numpy as jnp
from jax import lax
from jax.experimental import pallas as pl
from jax.experimental.pallas import tpu as pltpu
from jax.sharding import PartitionSpec as P


COHORTS = 16
LANES = 128
OWN_SHARE, OTHER_SHARE = 22, 21
BF16, F32 = jnp.bfloat16, jnp.float32
EXACT = lax.Precision.HIGHEST


def flip(size, stride):
    return [(i, i ^ stride) for i in range(size)]


def shift(size, step):
    return [(i, (i + step) % size) for i in range(size)]


def strides(size):
    return [1 << bit for bit in range(size.bit_length() - 1)]


def pick(array, index, axis):
    return lax.dynamic_index_in_dim(array, index, axis, keepdims=False)


def in_hbm(array):
    return pltpu.with_memory_space_constraint(array, pltpu.HBM)


def all_sum(value, size):
    for stride in strides(size):
        value = value + lax.ppermute(value, "samp", flip(size, stride))
    return value


def member_of(cohort, kind=F32):
    shape = (COHORTS, cohort.shape[-1])
    return (cohort == lax.broadcasted_iota(jnp.int32, shape, 0)).astype(kind)


def cohort_sums(member, values):
    values = values.reshape(-1, values.shape[-1])
    return lax.dot_general(
        member, values, (((1,), (1,)), ((), ())), precision=EXACT, preferred_element_type=F32
    )


def of_members(table, member):
    return lax.dot_general(
        table, member, (((0,), (0,)), ((), ())), precision=EXACT, preferred_element_type=F32
    )


def thirds(values):
    high = values.astype(BF16)
    values = values - high.astype(F32)
    mid = values.astype(BF16)
    return high, mid, (values - mid.astype(F32)).astype(BF16)


def score_kernel(cuts, weights_ref, dosages_ref, prior_ref, cohort_ref, *refs):
    *refs, weights, dosages, prior, cohort, acc, sems = refs
    part = lax.axis_index("var")
    size, parts, rows, samples = acc.shape
    share = size // parts
    member_ref, own_ref, *refs = refs
    sent_refs, sums_refs = refs[: parts - 1], refs[parts - 1 :]
    width = size * rows
    copies = []
    for k, (at, count) in enumerate(cuts):
        copies.append(
            (
                pltpu.make_async_copy(
                    weights_ref.at[pl.ds(at, count)], weights.at[pl.ds(at, count)], sems.at[0, k]
                ),
                pltpu.make_async_copy(
                    dosages_ref.at[:, pl.ds(at, count)],
                    dosages.at[:, pl.ds(at, count)],
                    sems.at[1, k],
                ),
            )
        )
        copies[k][0].start()
        copies[k][1].start()
    extra = pltpu.make_async_copy(prior_ref, prior, sems.at[2, 0])
    extra.start()
    known = pltpu.make_async_copy(cohort_ref, cohort, sems.at[2, 1])
    known.start()
    for k, (at, count) in enumerate(cuts):
        copies[k][0].wait()
        copies[k][1].wait()
        product = lax.dot_general(
            weights[pl.ds(at, count)],
            dosages[:, pl.ds(at, count)],
            (((0,), (1,)), ((), ())),
            preferred_element_type=F32,
        ).reshape(acc.shape)
        if k == 0:
            acc[...] = product
        else:
            acc[...] += product
    known.wait()
    member = member_of(cohort[...], BF16)
    member_ref[...] = member
    extra.wait()
    acc[pl.ds(part * share, share)] += prior[...].T.reshape(share, parts, rows, samples)

    def sums_of(values):
        pieces = thirds(values.reshape(size * rows, samples))
        return sum(
            lax.dot_general(member, x, (((1,), (1,)), ((), ())), preferred_element_type=F32)
            for x in pieces
        )

    values = acc[:, part]
    own_ref[...] = values
    sums_refs[0][:, :width] = sums_of(values)
    counts = jnp.sum(member.astype(F32), axis=1, keepdims=True)
    sums_refs[0][:, width:] = jnp.broadcast_to(counts, (COHORTS, LANES))
    for other in range(1, parts):
        values = acc[:, lax.rem(part + other, parts)]
        sums_refs[other][:, :width] = sums_of(values)
        sums_refs[other][:, width:] = jnp.zeros((COHORTS, LANES), F32)
        mean = jnp.mean(values, axis=2, keepdims=True)
        sent_refs[other - 1][...] = (values - mean).astype(BF16)


def center_kernel(own_ref, total_ref, member_ref, *refs):
    *others, out_ref = refs
    size, rows, samples = own_ref.shape
    width = size * rows
    table = -total_ref[:, :width] / total_ref[:, width : width + 1]
    scores = own_ref[...]
    for got_ref, theirs_ref in zip(others[::2], others[1::2]):
        scores += got_ref[...].astype(F32)
        table += jnp.sum(theirs_ref[:, :width], axis=0, keepdims=True) / samples
    member = member_ref[...]
    scores += lax.dot_general(
        jnp.concatenate(thirds(table), axis=0),
        jnp.concatenate([member] * 3, axis=0),
        (((0,), (0,)), ((), ())),
        preferred_element_type=F32,
    ).reshape(scores.shape)
    out_ref[...] = scores.astype(BF16)


def local_scores(dosages, weights, prior, cohort, size, parts):
    samples, variants = dosages.shape
    width = prior.shape[1]
    rows = width // size
    if rows % 16 == 0 and samples % LANES == 0 and variants % 256 == 0:
        step = min(896, variants)
        cuts = [(at, min(step, variants - at)) for at in range(0, variants, step)]
        vmem = pl.BlockSpec(memory_space=pltpu.VMEM)
        hbm = pl.BlockSpec(memory_space=pltpu.HBM)
        part_shape = (size, rows, samples)
        out = pl.pallas_call(
            functools.partial(score_kernel, cuts),
            out_shape=[
                pltpu.VMEM((COHORTS, samples), BF16),
                pltpu.VMEM(part_shape, F32),
                *[pltpu.VMEM(part_shape, BF16)] * (parts - 1),
                *[pltpu.VMEM((COHORTS, width + LANES), F32)] * parts,
            ],
            in_specs=[hbm] * 4,
            out_specs=[vmem] * (2 * parts + 1),
            scratch_shapes=[
                pltpu.VMEM((variants, width * parts), BF16),
                pltpu.VMEM((samples, variants), BF16),
                pltpu.VMEM((samples, width), F32),
                pltpu.VMEM((1, samples), jnp.int32),
                pltpu.VMEM((size, parts, rows, samples), F32),
                pltpu.SemaphoreType.DMA((3, len(cuts))),
            ],
            compiler_params=pltpu.CompilerParams(vmem_limit_bytes=16 << 20),
            name="scores",
        )(*map(in_hbm, (weights, dosages, prior, cohort)))
        return out[0], out[1], out[2 : parts + 1], out[parts + 1 :]
    part = lax.axis_index("var")
    scores = lax.dot_general(
        weights, dosages, (((0,), (1,)), ((), ())), preferred_element_type=F32
    ).reshape(size, parts, rows, samples)
    at = part * (size // parts)
    own = lax.dynamic_slice_in_dim(scores, at, size // parts, 0)
    own = own + prior.T.reshape(size // parts, parts, rows, samples)
    scores = lax.dynamic_update_slice_in_dim(scores, own, at, 0)
    by_part = [pick(scores, (part + other) % parts, 1) for other in range(parts)]
    member = member_of(cohort)
    counts = jnp.broadcast_to(jnp.sum(member, axis=1, keepdims=True), (COHORTS, LANES))
    sums = [
        jnp.concatenate([cohort_sums(member, x), counts * (k == 0)], axis=1)
        for k, x in enumerate(by_part)
    ]
    sent = [(x - jnp.mean(x, axis=2, keepdims=True)).astype(BF16) for x in by_part[1:]]
    return member.astype(BF16), by_part[0], sent, sums


def center(own, got, theirs, total, member):
    size, rows, samples = own.shape
    if rows % 16 == 0 and samples % LANES == 0:
        others = [x for pair in zip(got, theirs) for x in pair]
        return pl.pallas_call(
            center_kernel,
            out_shape=pltpu.VMEM(own.shape, BF16),
            compiler_params=pltpu.CompilerParams(vmem_limit_bytes=8 << 20),
            name="center",
        )(own, total, member, *others)
    width = size * rows
    table = -total[:, :width] / total[:, width : width + 1]
    table = table + jnp.sum(sum(theirs)[:, :width], axis=0)[None, :] / samples
    table = of_members(table, member.astype(F32)).reshape(own.shape)
    return (own + sum(x.astype(F32) for x in got) + table).astype(BF16)


def product_kernel(cuts, squares, standard_ref, expression_ref, sent_ref, mine_ref):
    bit = lax.axis_index("samp") & 1
    half, _, rows, samples = standard_ref.shape
    sent = standard_ref[:, 1 - bit].reshape(half * rows, samples)
    mine = standard_ref[:, bit].reshape(half * rows, samples)
    if squares:
        end = sum(cuts[-1][::2])
        first = lax.broadcasted_iota(jnp.int32, (half * rows, LANES), 1) < LANES // 2
        total = jnp.sum(sent.astype(F32) ** 2, axis=1, keepdims=True)
        high = total.astype(BF16).astype(F32)
        sent_ref[:, end:] = jnp.where(first, high, total - high).astype(BF16)
        total = jnp.sum(mine.astype(F32) ** 2, axis=1, keepdims=True)
        mine_ref[:, end:] = jnp.where(first, total, 0.0)
    both = jnp.concatenate([sent, mine], axis=0)
    for at, start, count in cuts:
        block = expression_ref[:, start : start + count]
        total = jnp.dot(both, block, preferred_element_type=F32)
        sent_ref[:, at : at + count] = total[: half * rows].astype(BF16)
        mine_ref[:, at : at + count] = total[half * rows :]


def products(standard, expression, at, count, squares):
    size, rows, samples = standard.shape
    halves = standard.reshape(size // 2, 2, rows, samples)
    if rows % 16 == 0 and samples % LANES == 0 and count % LANES == 0:
        step = 512
        cuts = [(k, at + k, min(step, count - k)) for k in range(0, count, step)]
        shape = (size // 2 * rows, count + LANES * squares)
        vmem = pl.BlockSpec(memory_space=pltpu.VMEM)
        return pl.pallas_call(
            functools.partial(product_kernel, cuts, squares),
            out_shape=[pltpu.VMEM(shape, BF16), pltpu.VMEM(shape, F32)],
            in_specs=[vmem, vmem],
            out_specs=[vmem, vmem],
            compiler_params=pltpu.CompilerParams(vmem_limit_bytes=12 << 20),
        )(halves, expression)
    expression = expression[:, at : at + count]
    results = []
    place = lax.axis_index("samp")
    for k in (1 - place & 1, place & 1):
        lhs = pick(halves, k, 1).reshape(-1, samples)
        result = jnp.dot(lhs, expression, preferred_element_type=F32)
        if squares:
            total = jnp.sum(lhs.astype(F32) ** 2, axis=1, keepdims=True)
            total = jnp.broadcast_to(total, (total.shape[0], LANES))
            first = jnp.arange(LANES) < LANES // 2
            if not results:
                high = lax.reduce_precision(total, 8, 7)
                total = jnp.where(first, high, total - high)
            else:
                total = jnp.where(first, total, 0.0)
            result = jnp.concatenate([result, total], axis=1)
        results.append(result)
    return results[0].astype(BF16), results[1]


def fold_kernel(shift, mine_ref, got_ref, sent_ref, kept_ref):
    bit = (lax.axis_index("samp") >> shift) & 1
    sent_ref[...] = (mine_ref[:, 1 - bit] + got_ref[:, 1 - bit].astype(F32)).astype(BF16)
    kept_ref[...] = mine_ref[:, bit] + got_ref[:, bit].astype(F32)


def fold(mine, got, stride):
    before, _, rows, width = mine.shape
    if rows % 16 == 0 and width % LANES == 0:
        vmem = pl.BlockSpec(memory_space=pltpu.VMEM)
        return pl.pallas_call(
            functools.partial(fold_kernel, stride.bit_length() - 1),
            out_shape=[pltpu.VMEM((before, rows, width), kind) for kind in (BF16, F32)],
            in_specs=[vmem, vmem],
            out_specs=[vmem, vmem],
            compiler_params=pltpu.CompilerParams(vmem_limit_bytes=4 << 20),
        )(mine, got)
    total = mine + got.astype(F32)
    bit = (lax.axis_index("samp") // stride) & 1
    return pick(total, 1 - bit, 1).astype(BF16), pick(total, bit, 1)


def scatter_sum(standard, expression, size, chunk):
    at, count, order = chunk
    rows = standard.shape[1]
    sent, mine = products(standard, expression, at, count, at == 0)
    width = sent.shape[1]
    left = strides(size)[::-1]
    for stride, coming in zip(order, [*order[1:], None]):
        left.remove(stride)
        got = lax.ppermute(sent, "samp", flip(size, stride))
        if coming is None:
            return mine.reshape(rows, width), got.reshape(rows, width)
        axis = left.index(coming)
        shape = (2**axis, 2, 2 ** (len(left) - axis - 1) * rows, width)
        sent, mine = fold(mine.reshape(shape), got.reshape(shape), coming)


def finish_kernel(plan, everyone, *refs):
    *refs, out_ref = refs
    parts = len(plan)
    terms = iter(zip(refs[::2], refs[1::2]))
    for k, chunks in enumerate(plan):
        part = lax.rem(lax.axis_index("var") + parts - k, parts)
        for at, count, _ in chunks:
            mine, got = next(terms)
            total = mine[...] + got[...].astype(F32)
            if at == 0:
                middle = count + LANES // 2
                squares = total[:, count : count + 1] + total[:, middle : middle + 1]
                spread = lax.rsqrt(squares / everyone + 1e-06) / everyone
            out_ref[part, :, at : at + count] = total[:, :count] * spread


def finish(cross, plan, everyone):
    rows = cross[0][0].shape[0]
    genes = sum(chunk[1] for chunk in plan[0])
    parts = len(plan)
    if rows % 16 == 0:
        vmem = pl.BlockSpec(memory_space=pltpu.VMEM)
        return pl.pallas_call(
            functools.partial(finish_kernel, plan, everyone),
            out_shape=jax.ShapeDtypeStruct((parts, rows, genes), F32),
            in_specs=[vmem] * (2 * len(cross)),
            out_specs=vmem,
            compiler_params=pltpu.CompilerParams(vmem_limit_bytes=12 << 20),
            name="finish",
        )(*[x for pair in cross for x in pair])
    result = jnp.zeros((parts, rows, genes), F32)
    cross = iter([mine + got.astype(F32) for mine, got in cross])
    for k, chunks in enumerate(plan):
        totals = [next(cross) for _ in chunks]
        count = chunks[0][1]
        squares = totals[0][:, count] + totals[0][:, count + LANES // 2]
        spread = lax.rsqrt(squares / everyone + 1e-06) / everyone
        values = jnp.concatenate([totals[0][:, :count], *totals[1:]], axis=1) * spread[:, None]
        result = lax.dynamic_update_slice_in_dim(result, values[None], (lax.axis_index("var") - k) % parts, 0)
    return result


def chunk_plan(size, parts, genes):
    near = strides(size)
    early, late = list(near), list(near)
    if size >= 16:
        early[2:4] = near[3], near[2]
        late[1:3] = near[2], near[1]
    tiles = genes // LANES
    cut = tiles * OWN_SHARE // 40 * LANES
    plan = [[(0, cut, early), (cut, genes - cut, near)]]
    for _ in range(1, parts):
        cut = tiles * OTHER_SHARE // 40 * LANES
        plan.append([(0, cut, near), (cut, genes - cut, late)])
    return plan


def shards(dosages, weights, prior, cohort, expression, *, size, parts):
    samples, width = prior.shape
    rows = width // size
    genes = expression.shape[1]
    cohort = cohort.reshape(1, samples)

    member, own, sent, sums = local_scores(dosages, weights, prior, cohort, size, parts)
    theirs = [lax.ppermute(sums[k], "var", shift(parts, k)) for k in range(1, parts)]
    got = [lax.ppermute(sent[k - 1], "var", shift(parts, k)) for k in range(1, parts)]
    total = all_sum(sum(theirs, sums[0]), size)

    standard = [center(own, got, theirs, total, member)]
    for k in range(1, parts):
        standard.append(lax.ppermute(standard[0], "var", shift(parts, k)))

    plan = chunk_plan(size, parts, genes)
    cross = [
        scatter_sum(standard[k], expression, size, chunk)
        for k, chunks in enumerate(plan)
        for chunk in chunks
    ]
    return finish(cross, plan, samples * size).reshape(parts * rows, genes)


def solution(mesh):
    size, parts = mesh.shape["samp"], mesh.shape["var"]
    placed = (P("samp", "var"), P("var", None), P("samp", "var"), P("samp", None), P("samp", "var"))
    return jax.shard_map(
        functools.partial(shards, size=size, parts=parts),
        mesh=mesh,
        in_specs=placed,
        out_specs=P("samp", "var"),
        check_vma=False,
    )
```
